32 devices in a mesh: dp: 8 (over z, y), section: 4 (over x, core).
Axes of the slice: x: 2, y: 2, z: 4, core: 2. Of those that a mesh axis runs over, the one named last changes fastest.
Arguments:
- slot_of_token: int32 [2, 1, 1024], P(None, None, 'dp'), may hold values from -1 to 127, as said below
- gate_prob: float32 [2, 1, 1024], P(None, None, 'dp'), may hold values from 0.2 to 1
- layer_input: bfloat16 [1, 1024, 7168], P(None, 'dp', 'section'), may hold values from -6 to 6
- preact: bfloat16 [1, 1024, 2048], P(None, 'dp', 'section'), may hold values from -6 to 6
- top_grad: bfloat16 [1, 1024, 3584], P(None, 'dp'), may hold values from -6 to 6
- w_up: bfloat16 [1024, 7168], P('dp', 'section'), may hold values from -0.09375 to 0.09375
- w_down: bfloat16 [1024, 7168], P('dp', 'section'), may hold values from -0.1875 to 0.1875
Outputs:
- grad_inputs: bfloat16 [1, 1024, 7168], P(None, 'dp', 'section')
- grad_up: float32 [1024, 7168], P('dp', 'section')
- grad_down: float32 [1024, 7168], P('dp', 'section')
The draws below stay inside these ranges and needn't reach their ends.
Inputs may be any that keep to these rules, and one draw needn't show every extreme that they name: `slot_of_token`: within one layer, one micro-batch and the 128 tokens of one data replica, the values other than -1 are distinct; -1 marks a token that is not routed to the expert or dropped.
All inputs are finite; a program needn't handle non-finite values.
Results may differ from the reference program's by a relative error of at most 0.0098.
Values may be sent and summed in bfloat16 or wider, within the bound.
No kernel may reach another device: no remote copies, remote signals or barrier semaphores. Data moves between devices by JAX's collectives and lax.ppermute only.
A program may use at most 128 MiB of HBM per device.

```python
import jax
import jax.numpy as jnp

D = 3584
F = 1024
SLOTS = 128
MB = 1
TOK = 128
LAYERS = 2
TOKENS = 1024
N_DP = 8


def draw_slot_of_token(key, part):
    blocks = LAYERS * MB * (TOKENS // TOK)
    block_keys = jax.random.split(key, blocks)

    def draw_block(block_key):
        shuffle_key, drop_key = jax.random.split(block_key)
        shuffled = jax.random.permutation(shuffle_key, SLOTS)[:TOK]
        kept_mask = jax.random.randint(drop_key, (TOK,), 0, 8) > 0
        return jnp.where(kept_mask, shuffled, -1).astype(jnp.int32)
    return jax.vmap(draw_block)(block_keys).reshape(LAYERS, MB, TOKENS)


def block_scale(rng, extent, cuts, low, largest):
    def one(axis_at, shards_of):
        heights = jax.random.uniform(jax.random.fold_in(jax.random.fold_in(rng, 6), axis_at), (shards_of,), jnp.float32, low / len(cuts), largest / len(cuts))
        return jnp.repeat(jnp.exp(heights), extent[axis_at] // shards_of).reshape((-1,) + (1,) * (len(extent) - axis_at - 1))

    factor_of = one(*cuts[0])
    for cut in cuts[1:]:
        factor_of = factor_of * one(*cut)
    return factor_of


def bell_draw(rng, shape, scale, bound, cuts=(), held_as=jnp.bfloat16):
    values = scale * jax.random.normal(rng, shape, jnp.float32)
    if cuts:
        values = values * block_scale(rng, shape, cuts, -0.22, 0.18)
    return jnp.clip(values, -bound, bound).astype(held_as)


def setup_inputs(seed: int = 0) -> dict:
    arg_keys = jax.random.split(jax.random.key(seed), 8)
    slot_of_token = draw_slot_of_token(jax.random.fold_in(arg_keys[7], 71), 0)
    gate_prob = jnp.clip(0.2 + 0.8 * jax.random.uniform(arg_keys[1], (LAYERS, MB, TOKENS), jnp.float32) ** block_scale(arg_keys[1], (LAYERS, MB, TOKENS), ((2, 8),), -0.2, 0.2), 0.2, 1.0)
    layer_input = bell_draw(arg_keys[2], (MB, TOKENS, LAYERS * D), 1.0, 6.0, ((1, 8), (2, 4)))
    preact = bell_draw(arg_keys[3], (MB, SLOTS * N_DP, LAYERS * F), 1.5, 6.0, ((1, 8), (2, 4)))
    top_grad = bell_draw(arg_keys[4], (MB, TOKENS, D), 1.0, 6.0, ((1, 8),))
    w_up = bell_draw(arg_keys[5], (F, LAYERS * D), D ** -0.5, 0.09375, ((0, 8), (1, 4)))
    w_down = bell_draw(arg_keys[6], (F, LAYERS * D), F ** -0.5, 0.1875, ((0, 8), (1, 4)))
    return dict(slot_of_token=slot_of_token, gate_prob=gate_prob, layer_input=layer_input, preact=preact, top_grad=top_grad, w_up=w_up, w_down=w_down)


def silu_slope(pre):
    sigmoid_val = jax.nn.sigmoid(pre)
    return sigmoid_val * (1.0 + pre * (1.0 - sigmoid_val))


def reference(slot_of_token, gate_prob, layer_input, preact, top_grad, w_up, w_down):
    groups = TOKENS // TOK
    grad_now = top_grad.reshape(MB, groups, TOK, D)
    slot_ids = jnp.arange(SLOTS, dtype=jnp.int32)
    inputs_out = []
    up_out = []
    down_out = []
    for layer in reversed(range(LAYERS)):
        slots_here = slot_of_token[layer].reshape(MB, groups, TOK)
        gates_here = gate_prob[layer].reshape(MB, groups, TOK)
        onehot = (slots_here[:, :, None, :] == slot_ids[None, None, :, None]).astype(jnp.float32)
        inputs_here = layer_input[:, :, layer * D:(layer + 1) * D].reshape(MB, groups, TOK, D)
        pre_here = preact[:, :, layer * F:(layer + 1) * F].reshape(MB * groups * SLOTS, F).astype(jnp.float32)
        up_here = w_up[:, layer * D:(layer + 1) * D]
        down_here = w_down[:, layer * D:(layer + 1) * D]
        scaled = (gates_here[..., None] * grad_now.astype(jnp.float32)).astype(jnp.bfloat16)
        slot_grad = jnp.einsum('mgst,mgtd->mgsd', onehot, scaled.astype(jnp.float32)).astype(jnp.bfloat16).reshape(-1, D)
        slot_inputs = jnp.einsum('mgst,mgtd->mgsd', onehot, inputs_here.astype(jnp.float32)).astype(jnp.bfloat16).reshape(-1, D)
        hidden_grad = jnp.dot(slot_grad, down_here.T, preferred_element_type=jnp.float32)
        pre_grad = (hidden_grad * silu_slope(pre_here)).astype(jnp.bfloat16)
        hidden = jax.nn.silu(pre_here).astype(jnp.bfloat16)
        slot_input_grad = jnp.dot(pre_grad, up_here, preferred_element_type=jnp.float32).astype(jnp.bfloat16)
        slot_input_grad = slot_input_grad.reshape(MB, groups, SLOTS, D)
        delta = jnp.einsum('mgst,mgsd->mgtd', onehot, slot_input_grad.astype(jnp.float32))
        grad_now = (grad_now.astype(jnp.float32) + delta).astype(jnp.bfloat16)
        inputs_out.append(grad_now.reshape(MB, TOKENS, D))
        up_out.append(jnp.dot(pre_grad.T, slot_inputs, preferred_element_type=jnp.float32))
        down_out.append(jnp.dot(hidden.T, slot_grad, preferred_element_type=jnp.float32))
    grad_inputs = jnp.concatenate(inputs_out[::-1], axis=2)
    grad_up = jnp.concatenate(up_out[::-1], axis=1)
    grad_down = jnp.concatenate(down_out[::-1], axis=1)
    return (grad_inputs, grad_up, grad_down)
```

```python
import jax
import jax.numpy as jnp
from jax import lax
from jax.sharding import PartitionSpec as P


def swapped(block, axis, apart):
    count = lax.axis_size(axis)
    route = []
    for low in range(count):
        high = low | 1 << apart
        if high != low and high < count:
            route += [(low, high), (high, low)]
    return lax.ppermute(block, axis, route)


def passed_along(shard, axis, by):
    count = lax.axis_size(axis)
    pairs = [(i, i + by) for i in range(count) if 0 <= i + by < count]
    return lax.ppermute(shard, axis, pairs)


def silu_slope(pre):
    sigmoid_val = jax.nn.sigmoid(pre)
    return sigmoid_val * (1.0 + pre * (1.0 - sigmoid_val))


def pick(stack, index):
    return lax.dynamic_index_in_dim(stack, index, 0, keepdims=False)


def blocks_to_owners(blocks):
    return lax.all_to_all(blocks, "dp", 0, 0, tiled=True)


def column_blocks(x):
    count = lax.axis_size("dp")
    split = x.reshape(x.shape[:-1] + (count, x.shape[-1] // count))
    return jnp.moveaxis(split, -2, 0)


def to_every(x):
    return jnp.broadcast_to(x[None], (lax.axis_size("dp"),) + x.shape)


def both_halves(mine, core_index):
    other = swapped(mine, "section", 0)
    return jnp.where(
        core_index == 0,
        jnp.concatenate([mine, other], -1),
        jnp.concatenate([other, mine], -1),
    )


def ring_order(count):
    width = 1 << ((count.bit_length() - 1) // 2)
    depth = count // width
    order = [z * width for z in range(depth)]
    for z in reversed(range(depth)):
        steps = list(range(1, width))
        order += [z * width + y for y in (steps if (depth - z) % 2 else steps[::-1])]
    return order


def ring_gather(shard):
    count = lax.axis_size("dp")
    order = ring_order(count)
    place = [0] * count
    for position, index in enumerate(order):
        place[index] = position
    here = jnp.asarray(place)[lax.axis_index("dp")]
    order_table = jnp.asarray(order)
    rows = shard.shape[0]
    half = rows // 2
    out = jnp.zeros((count, rows) + shard.shape[1:], shard.dtype)
    out = lax.dynamic_update_slice(out, shard[None], (lax.axis_index("dp"), 0, 0))
    ahead, behind = shard[:half], shard[half:]
    forth = [(order[k], order[(k + 1) % count]) for k in range(count)]
    back = [(high, low) for low, high in forth]
    for step in range(1, count):
        ahead = lax.ppermute(ahead, "dp", forth)
        behind = lax.ppermute(behind, "dp", back)
        out = lax.dynamic_update_slice(
            out, ahead[None], (order_table[(here - step) % count], 0, 0)
        )
        out = lax.dynamic_update_slice(
            out, behind[None], (order_table[(here + step) % count], half, 0)
        )
    return out.reshape((count * rows,) + shard.shape[1:])


def local(slot_of_token, gate_prob, layer_input, preact, top_grad, w_up, w_down):
    micro_count = layer_input.shape[0]
    token_rows = layer_input.shape[1]
    half_width = layer_input.shape[2]
    slot_count = preact.shape[1]
    section_index = lax.axis_index("section")
    pair_index = section_index // 2
    core_index = section_index % 2
    layer_count = lax.axis_size("section") // 2
    up_half, down_half = (
        ring_gather(w_up),
        ring_gather(w_down),
    )
    hidden_units = up_half.shape[0]
    pre_width = preact.shape[2]
    slope_all = silu_slope(both_halves(preact, core_index).astype(jnp.float32))
    hidden_here = jax.nn.silu(preact.astype(jnp.float32)).astype(jnp.bfloat16)
    slots_here = pick(slot_of_token, pair_index)
    gates_here = pick(gate_prob, pair_index)
    slot_ids = jnp.arange(slot_count, dtype=jnp.int32)
    onehot_all = (slots_here[:, None, :] == slot_ids[None, :, None]).astype(jnp.bfloat16)
    slot_inputs = jnp.einsum(
        "mst,mtd->msd", onehot_all, layer_input, preferred_element_type=jnp.float32
    ).astype(jnp.bfloat16)
    early = blocks_to_owners(
        jnp.concatenate([to_every(hidden_here), column_blocks(slot_inputs)], -1)
    )
    hidden_every = both_halves(early[..., :pre_width], core_index)
    top_half = lax.dynamic_slice_in_dim(top_grad, core_index * half_width, half_width, 2)
    tick_count = micro_count + layer_count - 1
    received = jnp.zeros((token_rows, half_width), jnp.bfloat16)
    grad_inputs = jnp.zeros_like(layer_input)
    pre_grads = jnp.zeros((micro_count, slot_count, hidden_units), jnp.bfloat16)
    slot_grads = jnp.zeros((micro_count, slot_count, half_width), jnp.bfloat16)
    for step_index in range(tick_count):
        micro_raw = step_index - (layer_count - 1 - pair_index)
        active = (micro_raw >= 0) & (micro_raw < micro_count)
        micro_now = jnp.clip(micro_raw, 0, micro_count - 1)
        incoming = jnp.where(pair_index == layer_count - 1, pick(top_half, micro_now), received)
        onehot = pick(onehot_all, micro_now)
        scaled = (pick(gates_here, micro_now)[:, None] * incoming.astype(jnp.float32)).astype(
            jnp.bfloat16
        )
        slot_grad = jnp.dot(onehot, scaled, preferred_element_type=jnp.float32).astype(jnp.bfloat16)
        partial_grad = lax.dot_general(
            slot_grad, down_half, (((1,), (1,)), ((), ())), preferred_element_type=jnp.float32
        )
        other_grad = swapped(partial_grad, "section", 0)
        hidden_grad = partial_grad + other_grad
        pre_grad = (hidden_grad * pick(slope_all, micro_now)).astype(jnp.bfloat16)
        slot_input_grad = jnp.dot(pre_grad, up_half, preferred_element_type=jnp.float32).astype(
            jnp.bfloat16
        )
        delta = lax.dot_general(
            onehot, slot_input_grad, (((0,), (0,)), ((), ())), preferred_element_type=jnp.float32
        )
        grad_new = (incoming.astype(jnp.float32) + delta).astype(jnp.bfloat16)
        grad_inputs = lax.dynamic_update_index_in_dim(
            grad_inputs, jnp.where(active, grad_new, pick(grad_inputs, micro_now)), micro_now, 0
        )
        pre_grads = lax.dynamic_update_index_in_dim(
            pre_grads, jnp.where(active, pre_grad, pick(pre_grads, micro_now)), micro_now, 0
        )
        slot_grads = lax.dynamic_update_index_in_dim(
            slot_grads, jnp.where(active, slot_grad, pick(slot_grads, micro_now)), micro_now, 0
        )
        received = passed_along(grad_new, "section", -2)
    pre_here = lax.dynamic_slice_in_dim(pre_grads, core_index * pre_width, pre_width, 2)
    late = blocks_to_owners(
        jnp.concatenate([to_every(pre_here), column_blocks(slot_grads)], -1)
    )
    pre_every = both_halves(late[..., :pre_width], core_index)
    up_columns = jnp.einsum(
        "nmsf,nmsd->fd", pre_every, early[..., pre_width:], preferred_element_type=jnp.float32
    )
    down_columns = jnp.einsum(
        "nmsf,nmsd->fd", hidden_every, late[..., pre_width:], preferred_element_type=jnp.float32
    )
    columns = jnp.concatenate([up_columns, down_columns], 1).astype(jnp.bfloat16)
    replicas = lax.axis_size("dp")
    owned = blocks_to_owners(columns.reshape(replicas, hidden_units // replicas, -1))
    owned = jnp.moveaxis(owned, 0, 1).astype(jnp.float32)
    block_width = half_width // replicas
    grad_up = owned[..., :block_width].reshape(-1, half_width)
    grad_down = owned[..., block_width:].reshape(-1, half_width)
    return (grad_inputs, grad_up, grad_down)


def solution(mesh):
    in_specs = (
        P(None, None, "dp"),
        P(None, None, "dp"),
        P(None, "dp", "section"),
        P(None, "dp", "section"),
        P(None, "dp", None),
        P("dp", "section"),
        P("dp", "section"),
    )
    out_specs = (P(None, "dp", "section"), P("dp", "section"), P("dp", "section"))
    return jax.shard_map(local, mesh=mesh, in_specs=in_specs, out_specs=out_specs, check_vma=False)
```

```python
import jax
import jax.numpy as jnp
from jax import lax
from jax.sharding import PartitionSpec as P


def swapped(block, axis, apart):
    count = lax.axis_size(axis)
    route = []
    for low in range(count):
        high = low | 1 << apart
        if high != low and high < count:
            route += [(low, high), (high, low)]
    return lax.ppermute(block, axis, route)


def passed_along(shard, axis, by):
    count = lax.axis_size(axis)
    pairs = [(i, i + by) for i in range(count) if 0 <= i + by < count]
    return lax.ppermute(shard, axis, pairs)


def silu_slope(pre):
    sigmoid_val = jax.nn.sigmoid(pre)
    return sigmoid_val * (1.0 + pre * (1.0 - sigmoid_val))


def pick(stack, index):
    return lax.dynamic_index_in_dim(stack, index, 0, keepdims=False)


def blocks_to_owners(blocks):
    return lax.all_to_all(blocks, "dp", 0, 0, tiled=True)


def column_blocks(x):
    count = lax.axis_size("dp")
    split = x.reshape(x.shape[:-1] + (count, x.shape[-1] // count))
    return jnp.moveaxis(split, -2, 0)


def to_every(x):
    return jnp.broadcast_to(x[None], (lax.axis_size("dp"),) + x.shape)


def both_halves(mine, core_index):
    other = swapped(mine, "section", 0)
    return jnp.where(
        core_index == 0,
        jnp.concatenate([mine, other], -1),
        jnp.concatenate([other, mine], -1),
    )


def ring_order(count):
    width = 1 << ((count.bit_length() - 1) // 2)
    depth = count // width
    order = [z * width for z in range(depth)]
    for z in reversed(range(depth)):
        steps = list(range(1, width))
        order += [z * width + y for y in (steps if (depth - z) % 2 else steps[::-1])]
    return order


def ring_gather(shard):
    count = lax.axis_size("dp")
    order = ring_order(count)
    table = [None] * count
    for position, index in enumerate(order):
        table[index] = [order[(position + step) % count] for step in range(count)]
    owners = lax.dynamic_index_in_dim(
        jnp.asarray(table, jnp.int32), lax.axis_index("dp"), 0, keepdims=False
    )
    rows = shard.shape[0]
    half = rows // 2
    out = to_every(shard)
    ahead, behind = shard[:half], shard[half:]
    forth = [(order[k], order[(k + 1) % count]) for k in range(count)]
    back = [(high, low) for low, high in forth]
    for step in range(1, count):
        ahead = lax.ppermute(ahead, "dp", forth)
        behind = lax.ppermute(behind, "dp", back)
        out = lax.dynamic_update_slice(
            out, ahead[None], (owners[count - step], 0, 0)
        )
        out = lax.dynamic_update_slice(
            out, behind[None], (owners[step], half, 0)
        )
    return out.reshape((count * rows,) + shard.shape[1:])


def local(slot_of_token, gate_prob, layer_input, preact, top_grad, w_up, w_down):
    micro_count = layer_input.shape[0]
    token_rows = layer_input.shape[1]
    half_width = layer_input.shape[2]
    slot_count = preact.shape[1]
    section_index = lax.axis_index("section")
    pair_index = section_index // 2
    core_index = section_index % 2
    layer_count = lax.axis_size("section") // 2
    up_half, down_half = (
        ring_gather(w_up),
        ring_gather(w_down),
    )
    hidden_units = up_half.shape[0]
    pre_width = preact.shape[2]
    slope_all = silu_slope(both_halves(preact, core_index).astype(jnp.float32))
    hidden_here = jax.nn.silu(preact.astype(jnp.float32)).astype(jnp.bfloat16)
    slots_here = pick(slot_of_token, pair_index)
    gates_here = pick(gate_prob, pair_index)
    slot_ids = jnp.arange(slot_count, dtype=jnp.int32)
    onehot_all = (slots_here[:, None, :] == slot_ids[None, :, None]).astype(jnp.bfloat16)
    slot_inputs = jnp.einsum(
        "mst,mtd->msd", onehot_all, layer_input, preferred_element_type=jnp.float32
    ).astype(jnp.bfloat16)
    early_blocks, up_half, down_half = lax.optimization_barrier(
        (
            jnp.concatenate([to_every(hidden_here), column_blocks(slot_inputs)], -1),
            up_half,
            down_half,
        )
    )
    early = blocks_to_owners(early_blocks)
    hidden_every = both_halves(early[..., :pre_width], core_index)
    top_half = lax.dynamic_slice_in_dim(top_grad, core_index * half_width, half_width, 2)
    tick_count = micro_count + layer_count - 1
    received = jnp.zeros((token_rows, half_width), jnp.bfloat16)
    grad_inputs = jnp.zeros_like(layer_input)
    pre_grads = jnp.zeros((micro_count, slot_count, hidden_units), jnp.bfloat16)
    slot_grads = jnp.zeros((micro_count, slot_count, half_width), jnp.bfloat16)
    for step_index in range(tick_count):
        micro_raw = step_index - (layer_count - 1 - pair_index)
        active = (micro_raw >= 0) & (micro_raw < micro_count)
        micro_now = jnp.clip(micro_raw, 0, micro_count - 1)
        incoming = jnp.where(pair_index == layer_count - 1, pick(top_half, micro_now), received)
        onehot = pick(onehot_all, micro_now)
        scaled = (pick(gates_here, micro_now)[:, None] * incoming.astype(jnp.float32)).astype(
            jnp.bfloat16
        )
        slot_grad = jnp.dot(onehot, scaled, preferred_element_type=jnp.float32).astype(jnp.bfloat16)
        partial_grad = lax.dot_general(
            slot_grad, down_half, (((1,), (1,)), ((), ())), preferred_element_type=jnp.float32
        )
        other_grad = swapped(partial_grad, "section", 0)
        hidden_grad = partial_grad + other_grad
        pre_grad = (hidden_grad * pick(slope_all, micro_now)).astype(jnp.bfloat16)
        slot_input_grad = jnp.dot(pre_grad, up_half, preferred_element_type=jnp.float32).astype(
            jnp.bfloat16
        )
        delta = lax.dot_general(
            onehot, slot_input_grad, (((0,), (0,)), ((), ())), preferred_element_type=jnp.float32
        )
        grad_new = (incoming.astype(jnp.float32) + delta).astype(jnp.bfloat16)
        grad_inputs = lax.dynamic_update_index_in_dim(
            grad_inputs, jnp.where(active, grad_new, pick(grad_inputs, micro_now)), micro_now, 0
        )
        pre_grads = lax.dynamic_update_index_in_dim(
            pre_grads, jnp.where(active, pre_grad, pick(pre_grads, micro_now)), micro_now, 0
        )
        slot_grads = lax.dynamic_update_index_in_dim(
            slot_grads, jnp.where(active, slot_grad, pick(slot_grads, micro_now)), micro_now, 0
        )
        received = passed_along(grad_new, "section", -2)
    pre_here = lax.dynamic_slice_in_dim(pre_grads, core_index * pre_width, pre_width, 2)
    late = blocks_to_owners(
        jnp.concatenate([to_every(pre_here), column_blocks(slot_grads)], -1)
    )
    pre_every = both_halves(late[..., :pre_width], core_index)
    up_columns = jnp.einsum(
        "nmsf,nmsd->fd", pre_every, early[..., pre_width:], preferred_element_type=jnp.float32
    )
    down_columns = jnp.einsum(
        "nmsf,nmsd->fd", hidden_every, late[..., pre_width:], preferred_element_type=jnp.float32
    )
    columns = jnp.concatenate([up_columns, down_columns], 1).astype(jnp.bfloat16)
    replicas = lax.axis_size("dp")
    owned = blocks_to_owners(columns.reshape(replicas, hidden_units // replicas, -1))
    owned = jnp.moveaxis(owned, 0, 1).astype(jnp.float32)
    block_width = half_width // replicas
    grad_up = owned[..., :block_width].reshape(-1, half_width)
    grad_down = owned[..., block_width:].reshape(-1, half_width)
    return (grad_inputs, grad_up, grad_down)


def solution(mesh):
    in_specs = (
        P(None, None, "dp"),
        P(None, None, "dp"),
        P(None, "dp", "section"),
        P(None, "dp", "section"),
        P(None, "dp", None),
        P("dp", "section"),
        P("dp", "section"),
    )
    out_specs = (P(None, "dp", "section"), P("dp", "section"), P("dp", "section"))
    return jax.shard_map(local, mesh=mesh, in_specs=in_specs, out_specs=out_specs, check_vma=False)
```
